8 devices in a mesh: dep: 2 (over z, y), col: 2 (over x), row: 2 (over core).
Axes of the slice: x: 2, y: 2, z: 1, core: 2. Of those that a mesh axis runs over, the one named last changes fastest.
Arguments:
- tokens: bfloat16 [8192, 1536], P(('dep', 'row'), 'col')
- w_up1: bfloat16 [1536, 8960], P('row', 'col')
- w_down1: bfloat16 [8960, 1536], P('row', 'col')
- w_up2: bfloat16 [1536, 8960], P('row', 'col')
- w_down2: bfloat16 [8960, 1536], P('row', 'col')
- grad_out: bfloat16 [8192, 1536], P(('dep', 'row'), 'col')
Outputs:
- output 1: bfloat16 [8192, 1536], P(('dep', 'row'), 'col')
- output 2: bfloat16 [8192, 1536], P(('dep', 'row'), 'col')
- output 3: float32 [1536, 8960], P('row', 'col')
- output 4: float32 [8960, 1536], P('row', 'col')
- output 5: float32 [1536, 8960], P('row', 'col')
- output 6: float32 [8960, 1536], P('row', 'col')
All inputs are finite; a program needn't handle non-finite values.
Results may differ from the reference program's by a relative error of at most 0.00525651.
Values are sent between devices in bfloat16 or wider.
A program may use at most 1 GiB of HBM per device.

```python
import math
import jax
import jax.numpy as jnp
from jax import lax

HIDDEN = 1536
FFN_DIM = 8960
TOKENS = 8192
ROW_BLOCK = math.gcd(TOKENS, 512)
NUM_BLOCKS = TOKENS // ROW_BLOCK


def setup_inputs(seed: int = 0) -> dict:
    keys = jax.random.split(jax.random.key(seed), 6)
    tokens = jax.random.normal(keys[0], (TOKENS, HIDDEN), jnp.float32)
    w_up1 = jax.random.normal(keys[1], (HIDDEN, FFN_DIM), jnp.float32) * HIDDEN ** -0.5
    w_down1 = jax.random.normal(keys[2], (FFN_DIM, HIDDEN), jnp.float32) * FFN_DIM ** -0.5
    w_up2 = jax.random.normal(keys[3], (HIDDEN, FFN_DIM), jnp.float32) * HIDDEN ** -0.5
    w_down2 = jax.random.normal(keys[4], (FFN_DIM, HIDDEN), jnp.float32) * FFN_DIM ** -0.5
    grad_out = jax.random.normal(keys[5], (TOKENS, HIDDEN), jnp.float32)
    return {
        "tokens": tokens.astype(jnp.bfloat16),
        "w_up1": w_up1.astype(jnp.bfloat16),
        "w_down1": w_down1.astype(jnp.bfloat16),
        "w_up2": w_up2.astype(jnp.bfloat16),
        "w_down2": w_down2.astype(jnp.bfloat16),
        "grad_out": grad_out.astype(jnp.bfloat16),
    }


def gelu_tanh(pre_act):
    return jax.nn.gelu(pre_act, approximate=True)


def gelu_grad(pre_act, grad_hidden):
    return jax.vjp(gelu_tanh, pre_act)[1](grad_hidden)[0]


def dot_last(left_op, right_op):
    return lax.dot_general(left_op, right_op, (((1,), (1,)), ((), ())), preferred_element_type=jnp.float32)


def dot_first(left_op, right_op):
    return lax.dot_general(left_op, right_op, (((0,), (0,)), ((), ())), preferred_element_type=jnp.float32)


def block_forward(block_in, w_up, w_down):
    pre_act = jnp.dot(block_in, w_up, preferred_element_type=jnp.float32)
    hidden = gelu_tanh(pre_act).astype(jnp.bfloat16)
    mlp_out = jnp.dot(hidden, w_down, preferred_element_type=jnp.float32)
    result = (block_in.astype(jnp.float32) + mlp_out).astype(jnp.bfloat16)
    return result, pre_act, hidden


def block_backward(block_in, pre_act, hidden, w_up, w_down, grad_res):
    grad_hidden = dot_last(grad_res, w_down)
    grad_pre = gelu_grad(pre_act, grad_hidden).astype(jnp.bfloat16)
    grad_in = (grad_res.astype(jnp.float32) + dot_last(grad_pre, w_up)).astype(jnp.bfloat16)
    grad_up = dot_first(block_in, grad_pre)
    grad_down = dot_first(hidden, grad_res)
    return grad_in, grad_up, grad_down


def reference(tokens, w_up1, w_down1, w_up2, w_down2, grad_out):
    def scan_step(grad_sums, inputs):
        tok_blk, grad_blk = inputs
        mid_acts, pre_first, hidden_first = block_forward(tok_blk, w_up1, w_down1)
        y_blk, pre_second, hidden_second = block_forward(mid_acts, w_up2, w_down2)
        grad_mid, grad_up2, grad_down2 = block_backward(mid_acts, pre_second, hidden_second, w_up2, w_down2, grad_blk)
        grad_in, grad_up1, grad_down1 = block_backward(tok_blk, pre_first, hidden_first, w_up1, w_down1, grad_mid)
        new_sums = (grad_sums[0] + grad_up1, grad_sums[1] + grad_down1, grad_sums[2] + grad_up2, grad_sums[3] + grad_down2)
        return new_sums, (y_blk, grad_in)

    zeros_up = jnp.zeros((HIDDEN, FFN_DIM), jnp.float32)
    zeros_down = jnp.zeros((FFN_DIM, HIDDEN), jnp.float32)
    tok_blocks = tokens.reshape(NUM_BLOCKS, ROW_BLOCK, HIDDEN)
    grad_blocks = grad_out.reshape(NUM_BLOCKS, ROW_BLOCK, HIDDEN)
    grad_sums, outs = lax.scan(scan_step, (zeros_up, zeros_down, zeros_up, zeros_down), (tok_blocks, grad_blocks))
    y_out = outs[0].reshape(TOKENS, HIDDEN)
    grad_x = outs[1].reshape(TOKENS, HIDDEN)
    return (y_out, grad_x, grad_sums[0], grad_sums[1], grad_sums[2], grad_sums[3])
```

```python
import jax
import jax.numpy as jnp
from jax import lax
from jax.sharding import PartitionSpec as P

CHUNKS = 2
LANES = 128


def gelu_tanh(pre_act):
    return jax.nn.gelu(pre_act, approximate=True)


def gelu_grad(pre_act, grad_hidden):
    return jax.vjp(gelu_tanh, pre_act)[1](grad_hidden)[0]


def dot(left_op, right_op):
    return jnp.dot(left_op, right_op, preferred_element_type=jnp.float32)


def dot_last(left_op, right_op):
    return lax.dot_general(left_op, right_op, (((1,), (1,)), ((), ())), preferred_element_type=jnp.float32)


def dot_first(left_op, right_op):
    return lax.dot_general(left_op, right_op, (((0,), (0,)), ((), ())), preferred_element_type=jnp.float32)


def swap(value, axis):
    return lax.ppermute(value, axis, [(0, 1), (1, 0)])


def swap_col_row(value):
    return lax.ppermute(value, ("col", "row"), [(0, 0), (1, 2), (2, 1), (3, 3)])


def half_of(value, index, axis):
    size = value.shape[axis] // 2
    return lax.dynamic_slice_in_dim(value, index * size, size, axis)


def gather_cols(value):
    return lax.all_gather(value, "col", axis=1, tiled=True)


def scatter_cols(value):
    return lax.psum_scatter(value, "col", scatter_dimension=1, tiled=True)


def up_weight(shard):
    return lax.all_gather(shard, "row", axis=0, tiled=True)


def down_weight(shard):
    return lax.all_gather(shard, "row", axis=1, tiled=True)


def hidden_of(acts, up):
    pre = dot(acts, up)
    return pre, gelu_tanh(pre).astype(jnp.bfloat16)


def grad_pre_of(pre, grad, down):
    return gelu_grad(pre, dot_last(grad, down)).astype(jnp.bfloat16)


def add_round(base, total):
    return (base.astype(jnp.float32) + total).astype(jnp.bfloat16)


def after(value, *others):
    return lax.optimization_barrier((value, *others))[0]


def solution(mesh):
    act_spec = P(("dep", "row"), "col")
    weight_spec = P("row", "col")

    def local_step(tokens, w_up1, w_down1, w_up2, w_down2, grad_out):
        dep = lax.axis_index("dep")
        row = lax.axis_index("row")
        chunk = tokens.shape[0] // CHUNKS
        ffn = w_down1.shape[0]
        window = -(-ffn // (2 * LANES)) * LANES
        start = dep * (ffn - window)
        skip = 2 * window - ffn

        def win(value, axis):
            return lax.dynamic_slice_in_dim(value, start, window, axis)

        def split(value):
            return [value[i * chunk:(i + 1) * chunk] for i in range(CHUNKS)]

        def window_sum(pairs, index, split_left):
            total = None
            for left, right in pairs:
                if split_left:
                    term = dot_first(half_of(left, index, 1), right)
                else:
                    term = dot_first(left, half_of(right, index, 1))
                total = term if total is None else total + term
            return total

        def row_sum(pairs, split_left):
            sent = swap(window_sum(pairs, 1 - row, split_left), "row")
            return window_sum(pairs, row, split_left) + sent

        def join(mine, axis):
            other = swap(mine, "dep")
            low = jnp.where(dep == 0, mine, other)
            high = jnp.where(dep == 0, other, mine)
            high = lax.slice_in_dim(high, skip, window, axis=axis)
            return jnp.concatenate([low, high], axis=axis)

        def weight_grads(acts, hids, gpres, grads, far):
            acts_far, hids_far, gpres_far, grads_far = far
            down = row_sum(list(zip([win(h, 1) for h in hids] + hids_far, grads + grads_far)), False)
            grad_down = join(swap_col_row(down), 0)
            up = row_sum(list(zip(acts + acts_far, [win(g, 1) for g in gpres] + gpres_far)), True)
            return join(up, 1), grad_down

        def far_side(acts, grads, up, down):
            acts_far = [swap(v, "dep") for v in acts]
            grads_far = [swap(v, "dep") for v in grads]
            up_win, down_win = win(up, 1), win(down, 0)
            hids, gpres = [], []
            for a, g in zip(acts_far, grads_far):
                pre, hid = hidden_of(a, up_win)
                hids.append(hid)
                gpres.append(grad_pre_of(pre, g, down_win))
            return acts_far, hids, gpres, grads_far

        x_own, g_own = split(tokens), split(grad_out)
        up1 = up_weight(w_up1)
        x_full = [gather_cols(v) for v in x_own]
        down1_shard = swap_col_row(w_down1)
        down1 = down_weight(down1_shard)
        down2_shard = swap_col_row(after(w_down2, down1_shard))
        pre1, hid1, z_own, z_full = [], [], [], []
        for i in range(CHUNKS):
            pre, hid = hidden_of(x_full[i], up1)
            pre1.append(pre)
            hid1.append(hid)
            if i == CHUNKS - 1:
                hid = after(hid, down2_shard)
            z_own.append(add_round(x_own[i], scatter_cols(dot(hid, down1))))
            z_full.append(gather_cols(z_own[i]))

        up2 = up_weight(w_up2)
        down2 = down_weight(down2_shard)
        g_full = [gather_cols(v) for v in g_own]
        hid2, gpre2, dz_own, dz_full = [], [], [], []
        for i in range(CHUNKS):
            pre, hid = hidden_of(z_full[i], up2)
            gpre = grad_pre_of(pre, g_full[i], down2)
            hid2.append(hid)
            gpre2.append(gpre)
            dz_own.append(add_round(g_own[i], scatter_cols(dot_last(gpre, up2))))
            dz_full.append(gather_cols(dz_own[i]))

        far2 = far_side(z_full, g_full, up2, down2)
        grad_up2, grad_down2 = weight_grads(z_full, hid2, gpre2, g_full, far2)

        gpre1, dx_own = [], []
        for i in range(CHUNKS):
            gpre = grad_pre_of(pre1[i], dz_full[i], down1)
            gpre1.append(gpre)
            dx_own.append(add_round(dz_own[i], scatter_cols(dot_last(gpre, up1))))

        y_own = []
        for i in range(CHUNKS):
            hid = after(hid2[i], dz_own[-1])
            y_own.append(add_round(z_own[i], scatter_cols(dot(hid, down2))))

        far1 = far_side(x_full, dz_full, up1, down1)
        grad_up1, grad_down1 = weight_grads(x_full, hid1, gpre1, dz_full, far1)
        return (jnp.concatenate(y_own, axis=0), jnp.concatenate(dx_own, axis=0), grad_up1, grad_down1, grad_up2, grad_down2)

    return jax.shard_map(local_step, mesh=mesh, in_specs=(act_spec, weight_spec, weight_spec, weight_spec, weight_spec, act_spec), out_specs=(act_spec, act_spec, weight_spec, weight_spec, weight_spec, weight_spec), check_vma=False)
```

```python
import jax
import jax.numpy as jnp
from jax import lax
from jax.sharding import PartitionSpec as P

LANES = 128


def gelu_tanh(pre_act):
    return jax.nn.gelu(pre_act, approximate=True)


def gelu_grad(pre_act, grad_hidden):
    return jax.vjp(gelu_tanh, pre_act)[1](grad_hidden)[0]


def dot(left_op, right_op):
    return jnp.dot(left_op, right_op, preferred_element_type=jnp.float32)


def dot_last(left_op, right_op):
    return lax.dot_general(left_op, right_op, (((1,), (1,)), ((), ())), preferred_element_type=jnp.float32)


def dot_first(left_op, right_op):
    return lax.dot_general(left_op, right_op, (((0,), (0,)), ((), ())), preferred_element_type=jnp.float32)


def swap(value, axis):
    return lax.ppermute(value, axis, [(0, 1), (1, 0)])


def half_of(value, index, axis):
    size = value.shape[axis] // 2
    return lax.dynamic_slice_in_dim(value, index * size, size, axis)


def gather_cols(value):
    return lax.all_gather(value, "col", axis=1, tiled=True)


def scatter_cols(value):
    return lax.psum_scatter(value, "col", scatter_dimension=1, tiled=True)


def in_order(index, mine, other, axis):
    low = jnp.where(index == 0, mine, other)
    high = jnp.where(index == 0, other, mine)
    return jnp.concatenate([low, high], axis=axis)


def hidden_of(acts, up):
    pre = dot(acts, up)
    return pre, gelu_tanh(pre).astype(jnp.bfloat16)


def grad_pre_of(pre, grad, down):
    return gelu_grad(pre, dot_last(grad, down)).astype(jnp.bfloat16)


def add_round(base, total):
    return (base.astype(jnp.float32) + total).astype(jnp.bfloat16)


def after(value, *others):
    return lax.optimization_barrier((value, *others))[0]


def solution(mesh):
    act_spec = P(("dep", "row"), "col")
    weight_spec = P("row", "col")

    def local_step(tokens, w_up1, w_down1, w_up2, w_down2, grad_out):
        dep = lax.axis_index("dep")
        col = lax.axis_index("col")
        row = lax.axis_index("row")
        chunk = tokens.shape[0] // 2
        ffn = w_down1.shape[0]
        window = -(-ffn // (2 * LANES)) * LANES
        start = dep * (ffn - window)
        skip = 2 * window - ffn
        last = [None]

        def run(fn, *args):
            if last[0] is not None:
                args, _ = lax.optimization_barrier((args, last[0]))
            out = fn(*args)
            last[0] = jax.tree.leaves(out)[-1]
            return out

        def win(value, axis):
            return lax.dynamic_slice_in_dim(value, start, window, axis)

        def split(value):
            return value[:chunk], value[chunk:]

        def hop(value):
            moved = lax.ppermute(value, ("dep", "col", "row"), [(1, 2), (2, 1), (5, 6), (6, 5)])
            return moved

        def hop_far(value):
            return lax.ppermute(value, ("dep", "col", "row"), [(1, 5), (5, 1), (2, 6), (6, 2)])

        def own_or(shard, moved):
            return jnp.where(col == row, shard, moved)

        def own_or_halves(shard, half, far):
            return own_or(shard, in_order(dep, half, far, 0))

        def join(mine, axis):
            other = swap(mine, "dep")
            low = jnp.where(dep == 0, mine, other)
            high = jnp.where(dep == 0, other, mine)
            high = lax.slice_in_dim(high, skip, window, axis=axis)
            return jnp.concatenate([low, high], axis=axis)

        def stack_win(near0, near1, far0, far1):
            return win(near0, 1), win(near1, 1), far0, far1

        def stack(*values):
            return jnp.concatenate(values, axis=0)

        def down_term(hids, grads, index):
            return sum(dot_first(h, half_of(g, index, 1)) for h, g in zip(hids, grads))

        def up_term(acts, gpres, index):
            return sum(dot_first(half_of(a, index, 1), g) for a, g in zip(acts, gpres))

        def plus(fn, left, right, index, received):
            return fn(left, right, index) + received

        x0, x1 = split(tokens)
        g0, g1 = split(grad_out)

        up1_other = swap(w_up1, "row")
        moved1 = hop(w_down1)
        xa0 = gather_cols(x0)
        xa1 = gather_cols(x1)
        up2_other = swap(after(w_up2, up1_other), "row")
        up1 = run(lambda a, b: in_order(row, a, b, 0), w_up1, up1_other)

        pre1_0, hid1_0 = run(hidden_of, xa0, up1)
        ga0 = gather_cols(after(g0, xa1))
        xf0 = swap(xa0, "dep")
        pre1_1, hid1_1 = run(hidden_of, xa1, up1)
        xf1 = swap(xa1, "dep")
        tile1 = run(own_or, w_down1, moved1)
        tile1_other = swap(tile1, "row")
        half2 = hop(half_of(after(w_down2, moved1), dep, 0))
        down1 = run(lambda a, b: in_order(row, a, b, 1), tile1, tile1_other)
        part0 = run(dot, hid1_0, down1)
        zs0 = scatter_cols(part0)
        part1 = run(dot, hid1_1, down1)
        zs1 = scatter_cols(part1)
        gf0 = swap(ga0, "dep")
        up2 = run(lambda a, b: in_order(row, a, b, 0), w_up2, up2_other)
        up1_win = run(lambda a: win(a, 1), up1)
        half2_far = hop_far(half2)
        hid1_f0 = run(hidden_of, xf0, up1_win)
        z0 = run(add_round, x0, zs0)
        za0 = gather_cols(z0)
        hid1_f1 = run(hidden_of, xf1, up1_win)
        tile2 = run(own_or_halves, w_down2, half2, half2_far)
        tile2_other = swap(tile2, "row")
        z1 = run(add_round, x1, zs1)
        za1 = gather_cols(z1)
        ga1 = gather_cols(after(g1, z1))
        down2 = run(lambda a, b: in_order(row, a, b, 1), tile2, tile2_other)

        zf0 = swap(za0, "dep")
        pre2, hid2_0 = run(hidden_of, za0, up2)
        gpre2_0 = run(grad_pre_of, pre2, ga0, down2)
        zf1 = swap(za1, "dep")
        ds0 = scatter_cols(run(dot_last, gpre2_0, up2))
        gf1 = swap(ga1, "dep")
        pre2, hid2_1 = run(hidden_of, za1, up2)
        gpre2_1 = run(grad_pre_of, pre2, ga1, down2)
        ds1 = scatter_cols(run(dot_last, gpre2_1, up2))

        up2_win = run(lambda a: win(a, 1), up2)
        pre2_f0, hid2_f0 = run(hidden_of, zf0, up2_win)
        pre2_f1, hid2_f1 = run(hidden_of, zf1, up2_win)
        hids2 = stack_win( hid2_0, hid2_1, hid2_f0, hid2_f1)
        grads2 = (ga0, ga1, gf0, gf1)
        sent = run(down_term, hids2, grads2, 1 - row)
        got = swap(sent, "row")
        dz0 = run(add_round, g0, ds0)
        dza0 = gather_cols(dz0)
        down_b = run(lambda *a: plus(down_term, *a), hids2, grads2, row, got)
        dz1 = run(add_round, g1, ds1)
        dza1 = gather_cols(dz1)
        down_b_moved = hop(after(down_b, dza1))
        down2_win = win(down2, 0)
        gpre2_f0 = run(grad_pre_of, pre2_f0, gf0, down2_win)
        gpre2_f1 = run(grad_pre_of, pre2_f1, gf1, down2_win)
        acts2 = (za0, za1, zf0, zf1)
        gpres2 = stack_win( gpre2_0, gpre2_1, gpre2_f0, gpre2_f1)

        dzf0 = swap(dza0, "dep")
        gpre1_0 = run(grad_pre_of, pre1_0, dza0, down1)
        xs0 = scatter_cols(run(dot_last, gpre1_0, up1))
        dzf1 = swap(dza1, "dep")
        gpre1_1 = run(grad_pre_of, pre1_1, dza1, down1)
        xs1 = scatter_cols(run(dot_last, gpre1_1, up1))

        down_b = run(lambda a, b: jnp.where(col == row, a, b), down_b, down_b_moved)
        grad_down2 = join(down_b, 0)
        sent = run(up_term, acts2, gpres2, 1 - row)
        got = swap(sent, "row")
        ys0 = scatter_cols(run(dot, hid2_0, down2))
        up_b = run(lambda *a: plus(up_term, *a), acts2, gpres2, row, got)
        grad_up2 = join(up_b, 1)

        grads1 = (dza0, dza1, dzf0, dzf1)
        hids1 = stack_win( hid1_0, hid1_1, hid1_f0[1], hid1_f1[1])
        sent = run(down_term, hids1, grads1, 1 - row)
        got = swap(sent, "row")
        down1_win = win(down1, 0)
        gpre1_f0 = run(grad_pre_of, hid1_f0[0], dzf0, down1_win)
        down_a = run(lambda *a: plus(down_term, *a), hids1, grads1, row, got)
        down_a_moved = hop(down_a)
        gpre1_f1 = run(grad_pre_of, hid1_f1[0], dzf1, down1_win)
        acts1 = (xa0, xa1, xf0, xf1)
        gpres1 = stack_win( gpre1_0, gpre1_1, gpre1_f0, gpre1_f1)
        sent = run(up_term, acts1, gpres1, 1 - row)
        got = swap(sent, "row")
        ys1 = scatter_cols(run(dot, hid2_1, down2))
        up_a = run(lambda *a: plus(up_term, *a), acts1, gpres1, row, got)
        grad_up1 = join(up_a, 1)
        down_a = run(lambda a, b: jnp.where(col == row, a, b), down_a, down_a_moved)
        grad_down1 = join(down_a, 0)
        grad_x = stack(add_round(dz0, xs0), add_round(dz1, xs1))
        y_out = stack(add_round(z0, ys0), add_round(z1, ys1))
        return y_out, grad_x, grad_up1, grad_down1, grad_up2, grad_down2

    return jax.shard_map(local_step, mesh=mesh, in_specs=(act_spec, weight_spec, weight_spec, weight_spec, weight_spec, act_spec), out_specs=(act_spec, act_spec, weight_spec, weight_spec, weight_spec, weight_spec), check_vma=False)
```

```python
import jax
import jax.numpy as jnp
from jax import lax
from jax.sharding import PartitionSpec as P

LANES = 128


def gelu_tanh(pre_act):
    return jax.nn.gelu(pre_act, approximate=True)


def gelu_grad(pre_act, grad_hidden):
    return jax.vjp(gelu_tanh, pre_act)[1](grad_hidden)[0]


def dot(left_op, right_op):
    return jnp.dot(left_op, right_op, preferred_element_type=jnp.float32)


def dot_last(left_op, right_op):
    return lax.dot_general(left_op, right_op, (((1,), (1,)), ((), ())), preferred_element_type=jnp.float32)


def dot_first(left_op, right_op):
    return lax.dot_general(left_op, right_op, (((0,), (0,)), ((), ())), preferred_element_type=jnp.float32)


def swap(value, axis):
    return lax.ppermute(value, axis, [(0, 1), (1, 0)])


def half_of(value, index, axis):
    size = value.shape[axis] // 2
    return lax.dynamic_slice_in_dim(value, index * size, size, axis)


def gather_cols(value):
    return lax.all_gather(value, "col", axis=1, tiled=True)


def scatter_cols(value):
    return lax.psum_scatter(value, "col", scatter_dimension=1, tiled=True)


def in_order(index, mine, other, axis):
    low = jnp.where(index == 0, mine, other)
    high = jnp.where(index == 0, other, mine)
    return jnp.concatenate([low, high], axis=axis)


def hidden_of(acts, up):
    pre = dot(acts, up)
    return pre, gelu_tanh(pre).astype(jnp.bfloat16)


def grad_pre_of(pre, grad, down):
    return gelu_grad(pre, dot_last(grad, down)).astype(jnp.bfloat16)


def add_round(base, total):
    return (base.astype(jnp.float32) + total).astype(jnp.bfloat16)


def after(value, *others):
    return lax.optimization_barrier((value, *others))[0]


def solution(mesh):
    act_spec = P(("dep", "row"), "col")
    weight_spec = P("row", "col")

    def local_step(tokens, w_up1, w_down1, w_up2, w_down2, grad_out):
        dep = lax.axis_index("dep")
        col = lax.axis_index("col")
        row = lax.axis_index("row")
        chunk = tokens.shape[0] // 2
        ffn = w_down1.shape[0]
        window = -(-ffn // (2 * LANES)) * LANES
        start = dep * (ffn - window)
        skip = 2 * window - ffn
        last = [None]

        def run(fn, *args):
            if last[0] is not None:
                args, _ = lax.optimization_barrier((args, last[0]))
            out = fn(*args)
            last[0] = jax.tree.leaves(out)[-1]
            return out

        def win(value, axis):
            return lax.dynamic_slice_in_dim(value, start, window, axis)

        def split(value):
            return value[:chunk], value[chunk:]

        def hop(value):
            moved = lax.ppermute(value, ("dep", "col", "row"), [(1, 2), (2, 1), (5, 6), (6, 5)])
            return moved

        def hop_far(value):
            return lax.ppermute(value, ("dep", "col", "row"), [(1, 5), (5, 1), (2, 6), (6, 2)])

        def own_or(shard, moved):
            return jnp.where(col == row, shard, moved)

        def own_or_halves(shard, half, far):
            return own_or(shard, in_order(dep, half, far, 0))

        def join(mine, axis):
            other = swap(mine, "dep")
            low = jnp.where(dep == 0, mine, other)
            high = jnp.where(dep == 0, other, mine)
            high = lax.slice_in_dim(high, skip, window, axis=axis)
            return jnp.concatenate([low, high], axis=axis)

        def down_term(hids, grads, index):
            near, far = ([dot_first(h, half_of(g, index, 1)) for h, g in zip(*p)] for p in zip(hids, grads))
            return (near[0] + near[1]) + (far[0] + far[1])

        def up_term(acts, gpres, index):
            near, far = ([dot_first(half_of(a, index, 1), g) for a, g in zip(*p)] for p in zip(acts, gpres))
            return (near[0] + near[1]) + (far[0] + far[1])

        def plus(fn, left, right, index, received):
            return fn(left, right, index) + received

        x0, x1 = split(tokens)
        g0, g1 = split(grad_out)

        up1_other = swap(w_up1, "row")
        moved1 = hop(w_down1)
        xa0 = gather_cols(x0)
        xa1 = gather_cols(x1)
        up2_other = swap(after(w_up2, up1_other), "row")
        up1 = run(lambda a, b: in_order(row, a, b, 0), w_up1, up1_other)

        pre1_0, hid1_0 = run(hidden_of, xa0, up1)
        ga0 = gather_cols(after(g0, xa1))
        xf0 = swap(xa0, "dep")
        pre1_1, hid1_1 = run(hidden_of, xa1, up1)
        xf1 = swap(xa1, "dep")
        tile1 = run(own_or, w_down1, moved1)
        tile1_other = swap(tile1, "row")
        half2 = hop(half_of(after(w_down2, moved1), dep, 0))
        down1 = run(lambda a, b: in_order(row, a, b, 1), tile1, tile1_other)
        part0 = run(dot, hid1_0, down1)
        zs0 = scatter_cols(part0)
        part1 = run(dot, hid1_1, down1)
        zs1 = scatter_cols(part1)
        gf0 = swap(ga0, "dep")
        up2 = run(lambda a, b: in_order(row, a, b, 0), w_up2, up2_other)
        half2_far = hop_far(half2)
        hid1_f0 = run(hidden_of, xf0, up1)
        z0 = run(add_round, x0, zs0)
        za0 = gather_cols(z0)
        hid1_f1 = run(hidden_of, xf1, up1)
        tile2 = run(own_or_halves, w_down2, half2, half2_far)
        tile2_other = swap(tile2, "row")
        z1 = run(add_round, x1, zs1)
        za1 = gather_cols(z1)
        ga1 = gather_cols(after(g1, z1))
        down2 = run(lambda a, b: in_order(row, a, b, 1), tile2, tile2_other)

        zf0 = swap(za0, "dep")
        pre2, hid2_0 = run(hidden_of, za0, up2)
        gpre2_0 = run(grad_pre_of, pre2, ga0, down2)
        zf1 = swap(after(za1, gpre2_0), "dep")
        part0 = run(dot_last, gpre2_0, up2)
        ds0 = scatter_cols(part0)
        gf1 = swap(after(ga1, part0), "dep")
        pre2, hid2_1 = run(hidden_of, za1, up2)
        gpre2_1 = run(grad_pre_of, pre2, ga1, down2)
        ds1 = scatter_cols(run(dot_last, gpre2_1, up2))

        up2_win = run(lambda a: win(a, 1), up2)
        pre2_f0, hid2_f0 = run(hidden_of, zf0, up2_win)
        pre2_f1, hid2_f1 = run(hidden_of, zf1, up2_win)
        dz0 = run(add_round, g0, ds0)
        dza0 = gather_cols(dz0)
        down2_win = win(down2, 0)
        gpre2_f0 = run(grad_pre_of, pre2_f0, gf0, down2_win)
        gpre2_f1 = run(grad_pre_of, pre2_f1, gf1, down2_win)
        acts2 = (za0, za1), (zf0, zf1)
        gpres2 = (win(gpre2_0, 1), win(gpre2_1, 1)), (gpre2_f0, gpre2_f1)
        sent = run(up_term, acts2, gpres2, 1 - row)
        got = swap(sent, "row")
        dz1 = run(add_round, g1, ds1)
        dza1 = gather_cols(dz1)
        dzf0 = swap(dza0, "dep")
        up_b = run(lambda *a: plus(up_term, *a), acts2, gpres2, row, got)
        dzf1 = swap(dza1, "dep")
        hids2 = (win(hid2_0, 1), win(hid2_1, 1)), (hid2_f0, hid2_f1)
        grads2 = (ga0, ga1), (gf0, gf1)
        sent = run(down_term, hids2, grads2, 1 - row)
        got = swap(sent, "row")
        grad_up2 = join(after(up_b, sent), 1)
        ys0 = scatter_cols(run(dot, hid2_0, down2))
        down_b = run(lambda *a: plus(down_term, *a), hids2, grads2, row, got)
        down_b_moved = hop(after(down_b, dza1))
        ys1 = scatter_cols(run(dot, hid2_1, down2))

        gpre1_0 = run(grad_pre_of, pre1_0, dza0, down1)
        xs0 = scatter_cols(run(dot_last, gpre1_0, up1))
        gpre1_1 = run(grad_pre_of, pre1_1, dza1, down1)
        grads1 = (dza0, dza1), (dzf0, dzf1)
        hids1 = (hid1_0, hid1_1), (hid1_f0[1], hid1_f1[1])
        sent = run(down_term, hids1, grads1, 1 - row)
        got = swap(sent, "row")
        xs1 = scatter_cols(run(dot_last, gpre1_1, up1))
        down_a = run(lambda *a: plus(down_term, *a), hids1, grads1, row, got)
        down_a_moved = hop(down_a)
        down_b = run(own_or, down_b, down_b_moved)
        grad_down2 = join(down_b, 0)
        gpre1_f0 = run(grad_pre_of, hid1_f0[0], dzf0, down1)
        gpre1_f1 = run(grad_pre_of, hid1_f1[0], dzf1, down1)
        acts1 = (xa0, xa1), (xf0, xf1)
        gpres1 = (gpre1_0, gpre1_1), (gpre1_f0, gpre1_f1)
        sent = run(up_term, acts1, gpres1, 1 - row)
        got = swap(sent, "row")
        y0 = run(add_round, z0, ys0)
        y1 = run(add_round, z1, ys1)
        dx0 = run(add_round, dz0, xs0)
        grad_up1 = run(lambda *a: plus(up_term, *a), acts1, gpres1, row, got)
        dx1 = run(add_round, dz1, xs1)
        grad_down1 = own_or(down_a, down_a_moved)
        y_out = jnp.concatenate([y0, y1], axis=0)
        grad_x = jnp.concatenate([dx0, dx1], axis=0)
        return y_out, grad_x, grad_up1, grad_down1, grad_up2, grad_down2

    return jax.shard_map(local_step, mesh=mesh, in_specs=(act_spec, weight_spec, weight_spec, weight_spec, weight_spec, act_spec), out_specs=(act_spec, act_spec, weight_spec, weight_spec, weight_spec, weight_spec), check_vma=False)
```

```python
import jax
import jax.numpy as jnp
from jax import lax
from jax.experimental import pallas as pl
from jax.experimental.pallas import tpu as pltpu
from jax.sharding import PartitionSpec as P

LANES = 128


def gelu_tanh(pre_act):
    return jax.nn.gelu(pre_act, approximate=True)


def gelu_grad(pre_act, grad_hidden):
    return jax.vjp(gelu_tanh, pre_act)[1](grad_hidden)[0]


def dot(left_op, right_op):
    return jnp.dot(left_op, right_op, preferred_element_type=jnp.float32)


def dot_last(left_op, right_op):
    return lax.dot_general(left_op, right_op, (((1,), (1,)), ((), ())), preferred_element_type=jnp.float32)


def dot_first(left_op, right_op):
    return lax.dot_general(left_op, right_op, (((0,), (0,)), ((), ())), preferred_element_type=jnp.float32)


def swap(value, axis):
    return lax.ppermute(value, axis, [(0, 1), (1, 0)])


def half_of(value, index, axis):
    size = value.shape[axis] // 2
    return lax.dynamic_slice_in_dim(value, index * size, size, axis)


def gather_cols(value):
    return lax.all_gather(value, "col", axis=1, tiled=True)


def scatter_cols(value):
    return lax.psum_scatter(value, "col", scatter_dimension=1, tiled=True)


def in_order(index, mine, other, axis):
    low = jnp.where(index == 0, mine, other)
    high = jnp.where(index == 0, other, mine)
    return jnp.concatenate([low, high], axis=axis)


def hidden_of(acts, up):
    pre = dot(acts, up)
    return gelu_grad(pre, jnp.ones_like(pre)), gelu_tanh(pre).astype(jnp.bfloat16)


def grad_pre_of(slope, grad, down):
    return (dot_last(grad, down) * slope).astype(jnp.bfloat16)


def add_round(base, total):
    return (base.astype(jnp.float32) + total).astype(jnp.bfloat16)


def after(value, *others):
    return lax.optimization_barrier((value, *others))[0]


def token_sum_kernel(index_ref, *refs):
    lefts, rights, rest = refs[:4], refs[4:8], refs[8:]
    terms = [dot_first(left[...], right[...]) for left, right in zip(lefts, rights)]
    total = (terms[0] + terms[1]) + (terms[2] + terms[3])
    out = rest[-1]
    if len(rest) == 2:
        total = total + rest[0][...]
    out[...] = total


def tile_of(size):
    return max(t for t in range(LANES, 897, LANES) if size % t == 0)


def token_sum(lefts, rights, index, received, halves_left):
    depth = lefts[0].shape[0]
    whole, halved = (rights, lefts) if halves_left else (lefts, rights)
    size, half = whole[0].shape[1], halved[0].shape[1] // 2
    tile = tile_of(size)
    whole_spec = pl.BlockSpec((depth, tile), lambda j, s: (0, j))
    half_spec = pl.BlockSpec((depth, half), lambda j, s: (0, s[0]))
    if halves_left:
        shape, out_spec = (half, size), pl.BlockSpec((half, tile), lambda j, s: (0, j))
        specs = [half_spec] * 4 + [whole_spec] * 4
    else:
        shape, out_spec = (size, half), pl.BlockSpec((tile, half), lambda j, s: (j, 0))
        specs = [whole_spec] * 4 + [half_spec] * 4
    specs = specs + [out_spec] * len(received)
    flops = 2 * 4 * depth * size * half
    moved = 4 * depth * (size + half) * 2 + (1 + len(received)) * size * half * 4
    return pl.pallas_call(
        token_sum_kernel,
        out_shape=jax.ShapeDtypeStruct(shape, jnp.float32),
        grid_spec=pltpu.PrefetchScalarGridSpec(num_scalar_prefetch=1, grid=(size // tile,), in_specs=specs, out_specs=out_spec),
        compiler_params=pltpu.CompilerParams(vmem_limit_bytes=60 * 1024 * 1024, dimension_semantics=("arbitrary",)),
        cost_estimate=pl.CostEstimate(flops=flops, bytes_accessed=moved, transcendentals=0),
        name="token_sum_up" if halves_left else "token_sum_down",
    )(jnp.reshape(index, (1,)).astype(jnp.int32), *lefts, *rights, *received)


def solution(mesh):
    act_spec = P(("dep", "row"), "col")
    weight_spec = P("row", "col")

    def local_step(tokens, w_up1, w_down1, w_up2, w_down2, grad_out):
        dep = lax.axis_index("dep")
        col = lax.axis_index("col")
        row = lax.axis_index("row")
        chunk = tokens.shape[0] // 2
        ffn = w_down1.shape[0]
        window = -(-ffn // (2 * LANES)) * LANES
        start = dep * (ffn - window)
        skip = 2 * window - ffn
        last = [None]

        def run(fn, *args):
            if last[0] is not None:
                args, _ = lax.optimization_barrier((args, last[0]))
            out = fn(*args)
            last[0] = jax.tree.leaves(out)[-1]
            return out

        def win(value, axis):
            return lax.dynamic_slice_in_dim(value, start, window, axis)

        def split(value):
            return value[:chunk], value[chunk:]

        def hop(value):
            moved = lax.ppermute(value, ("dep", "col", "row"), [(1, 2), (2, 1), (5, 6), (6, 5)])
            return moved

        def hop_far(value):
            return lax.ppermute(value, ("dep", "col", "row"), [(1, 5), (5, 1), (2, 6), (6, 2)])

        def own_or(shard, moved):
            return jnp.where(col == row, shard, moved)

        def own_or_halves(shard, half, far):
            return own_or(shard, in_order(dep, half, far, 0))

        def join(mine, axis):
            other = swap(mine, "dep")
            low = jnp.where(dep == 0, mine, other)
            high = jnp.where(dep == 0, other, mine)
            high = lax.slice_in_dim(high, skip, window, axis=axis)
            return jnp.concatenate([low, high], axis=axis)

        def down_term(hids, grads, index, *received):
            return token_sum(hids[0] + hids[1], grads[0] + grads[1], index, received, False)

        def up_term(acts, gpres, index, *received):
            return token_sum(acts[0] + acts[1], gpres[0] + gpres[1], index, received, True)

        x0, x1 = split(tokens)
        g0, g1 = split(grad_out)

        up1_other = swap(w_up1, "row")
        moved1 = hop(w_down1)
        xa0 = gather_cols(x0)
        xa1 = gather_cols(x1)
        up2_other = swap(after(w_up2, up1_other), "row")
        up1 = run(lambda a, b: in_order(row, a, b, 0), w_up1, up1_other)

        pre1_0, hid1_0 = run(hidden_of, xa0, up1)
        ga0 = gather_cols(after(g0, xa1))
        xf0 = swap(xa0, "dep")
        pre1_1, hid1_1 = run(hidden_of, xa1, up1)
        xf1 = swap(xa1, "dep")
        tile1 = run(own_or, w_down1, moved1)
        tile1_other = swap(tile1, "row")
        half2 = hop(half_of(after(w_down2, moved1), dep, 0))
        down1 = run(lambda a, b: in_order(row, a, b, 1), tile1, tile1_other)
        part0 = run(dot, hid1_0, down1)
        zs0 = scatter_cols(part0)
        part1 = run(dot, hid1_1, down1)
        zs1 = scatter_cols(part1)
        gf0 = swap(ga0, "dep")
        up2 = run(lambda a, b: in_order(row, a, b, 0), w_up2, up2_other)
        half2_far = hop_far(half2)
        hid1_f0 = run(hidden_of, xf0, up1)
        z0 = run(add_round, x0, zs0)
        za0 = gather_cols(z0)
        hid1_f1 = run(hidden_of, xf1, up1)
        tile2 = run(own_or_halves, w_down2, half2, half2_far)
        tile2_other = swap(tile2, "row")
        z1 = run(add_round, x1, zs1)
        za1 = gather_cols(z1)
        ga1 = gather_cols(after(g1, z1))
        down2 = run(lambda a, b: in_order(row, a, b, 1), tile2, tile2_other)

        zf0 = swap(za0, "dep")
        pre2, hid2_0 = run(hidden_of, za0, up2)
        gpre2_0 = run(grad_pre_of, pre2, ga0, down2)
        zf1 = swap(after(za1, gpre2_0), "dep")
        part0 = run(dot_last, gpre2_0, up2)
        ds0 = scatter_cols(part0)
        gf1 = swap(after(ga1, part0), "dep")
        pre2, hid2_1 = run(hidden_of, za1, up2)
        gpre2_1 = run(grad_pre_of, pre2, ga1, down2)
        ds1 = scatter_cols(run(dot_last, gpre2_1, up2))

        up2_win = run(lambda a: win(a, 1), up2)
        pre2_f0, hid2_f0 = run(hidden_of, zf0, up2_win)
        pre2_f1, hid2_f1 = run(hidden_of, zf1, up2_win)
        dz0 = run(add_round, g0, ds0)
        dza0 = gather_cols(dz0)
        down2_win = win(down2, 0)
        gpre2_f0 = run(grad_pre_of, pre2_f0, gf0, down2_win)
        gpre2_f1 = run(grad_pre_of, pre2_f1, gf1, down2_win)
        acts2 = (za0, za1), (zf0, zf1)
        gpres2 = (win(gpre2_0, 1), win(gpre2_1, 1)), (gpre2_f0, gpre2_f1)
        sent = run(up_term, acts2, gpres2, 1 - row)
        got = swap(sent, "row")
        dz1 = run(add_round, g1, ds1)
        dza1 = gather_cols(dz1)
        up_b = run(up_term, acts2, gpres2, row, got)
        hids2 = (win(hid2_0, 1), win(hid2_1, 1)), (hid2_f0, hid2_f1)
        grads2 = (ga0, ga1), (gf0, gf1)
        sent = run(down_term, hids2, grads2, 1 - row)
        got = swap(sent, "row")
        dzf0 = swap(dza0, "dep")
        ys0 = scatter_cols(run(dot, hid2_0, down2))
        down_b = run(down_term, hids2, grads2, row, got)
        dzf1 = swap(after(dza1, down_b), "dep")
        down_b_moved = hop(after(down_b, dza1))
        ys1 = scatter_cols(run(dot, hid2_1, down2))

        gpre1_0 = run(grad_pre_of, pre1_0, dza0, down1)
        grad_up2 = join(after(up_b, gpre1_0), 1)
        xs0 = scatter_cols(run(dot_last, gpre1_0, up1))
        gpre1_1 = run(grad_pre_of, pre1_1, dza1, down1)
        grads1 = (dza0, dza1), (dzf0, dzf1)
        hids1 = (hid1_0, hid1_1), (hid1_f0[1], hid1_f1[1])
        sent = run(down_term, hids1, grads1, 1 - row)
        got = swap(sent, "row")
        xs1 = scatter_cols(run(dot_last, gpre1_1, up1))
        down_a = run(down_term, hids1, grads1, row, got)
        down_a_moved = hop(down_a)
        down_b = run(own_or, down_b, down_b_moved)
        grad_down2 = join(down_b, 0)
        gpre1_f0 = run(grad_pre_of, hid1_f0[0], dzf0, down1)
        gpre1_f1 = run(grad_pre_of, hid1_f1[0], dzf1, down1)
        acts1 = (xa0, xa1), (xf0, xf1)
        gpres1 = (gpre1_0, gpre1_1), (gpre1_f0, gpre1_f1)
        sent = run(up_term, acts1, gpres1, 1 - row)
        got = swap(sent, "row")
        y0 = run(add_round, z0, ys0)
        y1 = run(add_round, z1, ys1)
        dx0 = run(add_round, dz0, xs0)
        grad_up1 = run(up_term, acts1, gpres1, row, got)
        dx1 = run(add_round, dz1, xs1)
        grad_down1 = own_or(down_a, down_a_moved)
        y_out = jnp.concatenate([y0, y1], axis=0)
        grad_x = jnp.concatenate([dx0, dx1], axis=0)
        return y_out, grad_x, grad_up1, grad_down1, grad_up2, grad_down2

    return jax.shard_map(local_step, mesh=mesh, in_specs=(act_spec, weight_spec, weight_spec, weight_spec, weight_spec, act_spec), out_specs=(act_spec, act_spec, weight_spec, weight_spec, weight_spec, weight_spec), check_vma=False)
```

```python
import jax
import jax.numpy as jnp
from jax import lax
from jax.experimental import pallas as pl
from jax.experimental.pallas import tpu as pltpu
from jax.sharding import PartitionSpec as P

LANES = 128


def gelu_tanh(pre_act):
    return jax.nn.gelu(pre_act, approximate=True)


def gelu_grad(pre_act, grad_hidden):
    return jax.vjp(gelu_tanh, pre_act)[1](grad_hidden)[0]


def dot(left_op, right_op):
    return jnp.dot(left_op, right_op, preferred_element_type=jnp.float32)


def dot_last(left_op, right_op):
    return lax.dot_general(left_op, right_op, (((1,), (1,)), ((), ())), preferred_element_type=jnp.float32)


def dot_first(left_op, right_op):
    return lax.dot_general(left_op, right_op, (((0,), (0,)), ((), ())), preferred_element_type=jnp.float32)


def swap(value, axis):
    return lax.ppermute(value, axis, [(0, 1), (1, 0)])


def half_of(value, index, axis):
    size = value.shape[axis] // 2
    return lax.dynamic_slice_in_dim(value, index * size, size, axis)


def gather_cols(value):
    return lax.all_gather(value, "col", axis=1, tiled=True)


def scatter_cols(value):
    return lax.psum_scatter(value, "col", scatter_dimension=1, tiled=True)


def in_order(index, mine, other, axis):
    low = jnp.where(index == 0, mine, other)
    high = jnp.where(index == 0, other, mine)
    return jnp.concatenate([low, high], axis=axis)


def hidden_of(acts, up):
    pre = dot(acts, up)
    return gelu_grad(pre, jnp.ones_like(pre)), gelu_tanh(pre).astype(jnp.bfloat16)


def grad_pre_of(slope, grad, down):
    return (dot_last(grad, down) * slope).astype(jnp.bfloat16)


def hidden_and_pre(acts, up):
    pre = dot(acts, up)
    return pre, gelu_tanh(pre).astype(jnp.bfloat16)


def grad_pre_from(pre, grad, down):
    return gelu_grad(pre, dot_last(grad, down)).astype(jnp.bfloat16)


def add_round(base, total):
    return (base.astype(jnp.float32) + total).astype(jnp.bfloat16)


def after(value, *others):
    return lax.optimization_barrier((value, *others))[0]


def token_sum_kernel(index_ref, *refs):
    lefts, rights, rest = refs[:4], refs[4:8], refs[8:]
    terms = [dot_first(left[...], right[...]) for left, right in zip(lefts, rights)]
    total = (terms[0] + terms[1]) + (terms[2] + terms[3])
    out = rest[-1]
    if len(rest) == 2:
        total = total + rest[0][...]
    out[...] = total


def tile_of(size):
    return max(t for t in range(LANES, 897, LANES) if size % t == 0)


def token_sum(lefts, rights, index, received, halves_left):
    depth = lefts[0].shape[0]
    whole, halved = (rights, lefts) if halves_left else (lefts, rights)
    size, half = whole[0].shape[1], halved[0].shape[1] // 2
    tile = tile_of(size)
    whole_spec = pl.BlockSpec((depth, tile), lambda j, s: (0, j))
    half_spec = pl.BlockSpec((depth, half), lambda j, s: (0, s[0]))
    if halves_left:
        shape, out_spec = (half, size), pl.BlockSpec((half, tile), lambda j, s: (0, j))
        specs = [half_spec] * 4 + [whole_spec] * 4
    else:
        shape, out_spec = (size, half), pl.BlockSpec((tile, half), lambda j, s: (j, 0))
        specs = [whole_spec] * 4 + [half_spec] * 4
    specs = specs + [out_spec] * len(received)
    flops = 2 * 4 * depth * size * half
    moved = 4 * depth * (size + half) * 2 + (1 + len(received)) * size * half * 4
    return pl.pallas_call(
        token_sum_kernel,
        out_shape=jax.ShapeDtypeStruct(shape, jnp.float32),
        grid_spec=pltpu.PrefetchScalarGridSpec(num_scalar_prefetch=1, grid=(size // tile,), in_specs=specs, out_specs=out_spec),
        compiler_params=pltpu.CompilerParams(vmem_limit_bytes=60 * 1024 * 1024, dimension_semantics=("arbitrary",)),
        cost_estimate=pl.CostEstimate(flops=flops, bytes_accessed=moved, transcendentals=0),
        name="token_sum_up" if halves_left else "token_sum_down",
    )(jnp.reshape(index, (1,)).astype(jnp.int32), *lefts, *rights, *received)


def solution(mesh):
    act_spec = P(("dep", "row"), "col")
    weight_spec = P("row", "col")

    def local_step(tokens, w_up1, w_down1, w_up2, w_down2, grad_out):
        dep = lax.axis_index("dep")
        col = lax.axis_index("col")
        row = lax.axis_index("row")
        chunk = tokens.shape[0] // 2
        ffn = w_down1.shape[0]
        window = -(-ffn // (2 * LANES)) * LANES
        start = dep * (ffn - window)
        skip = 2 * window - ffn
        last = [None]

        def run(fn, *args):
            if last[0] is not None:
                args, _ = lax.optimization_barrier((args, last[0]))
            out = fn(*args)
            last[0] = jax.tree.leaves(out)[-1]
            return out

        def win(value, axis):
            return lax.dynamic_slice_in_dim(value, start, window, axis)

        def split(value):
            return value[:chunk], value[chunk:]

        def hop(value):
            moved = lax.ppermute(value, ("dep", "col", "row"), [(1, 2), (2, 1), (5, 6), (6, 5)])
            return moved

        def hop_far(value):
            return lax.ppermute(value, ("dep", "col", "row"), [(1, 5), (5, 1), (2, 6), (6, 2)])

        def own_or(shard, moved):
            return jnp.where(col == row, shard, moved)

        def own_or_halves(shard, half, far):
            return own_or(shard, in_order(dep, half, far, 0))

        def join(mine, axis):
            other = swap(mine, "dep")
            low = jnp.where(dep == 0, mine, other)
            high = jnp.where(dep == 0, other, mine)
            high = lax.slice_in_dim(high, skip, window, axis=axis)
            return jnp.concatenate([low, high], axis=axis)

        def down_term(hids, grads, index, *received):
            return token_sum(hids[0] + hids[1], grads[0] + grads[1], index, received, False)

        def up_term(acts, gpres, index, *received):
            return token_sum(acts[0] + acts[1], gpres[0] + gpres[1], index, received, True)

        x0, x1 = split(tokens)
        g0, g1 = split(grad_out)

        up1_other = swap(w_up1, "row")
        half1 = hop(half_of(w_down1, dep, 0))
        xa0 = gather_cols(x0)
        xa1 = gather_cols(x1)
        up2_other = swap(after(w_up2, up1_other), "row")
        up1 = run(lambda a, b: in_order(row, a, b, 0), w_up1, up1_other)

        pre1_0, hid1_0 = run(hidden_of, xa0, up1)
        ga0 = gather_cols(after(g0, xa0))
        xf0 = swap(xa0, "dep")
        half1_far = hop_far(half1)
        pre1_1, hid1_1 = run(hidden_of, xa1, up1)
        xf1 = swap(xa1, "dep")
        tile1 = run(own_or_halves, w_down1, half1, half1_far)
        tile1_other = swap(tile1, "row")
        half2 = hop(half_of(after(w_down2, half1_far), dep, 0))
        down1 = run(lambda a, b: in_order(row, a, b, 1), tile1, tile1_other)
        part0 = run(dot, hid1_0, down1)
        zs0 = scatter_cols(part0)
        part1 = run(dot, hid1_1, down1)
        zs1 = scatter_cols(part1)
        gf0 = swap(ga0, "dep")
        up2 = run(lambda a, b: in_order(row, a, b, 0), w_up2, up2_other)
        half2_far = hop_far(half2)
        hid1_f0 = run(hidden_of, xf0, up1)
        z0 = run(add_round, x0, zs0)
        za0 = gather_cols(z0)
        hid1_f1 = run(hidden_of, xf1, up1)
        tile2 = run(own_or_halves, w_down2, half2, half2_far)
        tile2_other = swap(tile2, "row")
        z1 = run(add_round, x1, zs1)
        za1 = gather_cols(z1)
        ga1 = gather_cols(after(g1, z1))
        down2 = run(lambda a, b: in_order(row, a, b, 1), tile2, tile2_other)

        up2_win = run(lambda a: win(a, 1), up2)
        down2_win = run(lambda a: win(a, 0), down2)
        za0 = after(za0, down2_win)

        zf0 = swap(za0, "dep")
        pre2, hid2_0 = run(hidden_and_pre, za0, up2)
        gpre2_0 = run(grad_pre_from, pre2, ga0, down2)
        zf1 = swap(after(za1, gpre2_0), "dep")
        part0 = run(dot_last, gpre2_0, up2)
        ds0 = scatter_cols(part0)
        gf1 = swap(after(ga1, part0), "dep")
        pre2, hid2_1 = run(hidden_and_pre, za1, up2)
        gpre2_1 = run(grad_pre_from, pre2, ga1, down2)
        part1 = run(dot_last, gpre2_1, up2)
        ds1 = scatter_cols(part1)

        pre2_f0, hid2_f0 = run(hidden_of, zf0, up2_win)
        pre2_f1, hid2_f1 = run(hidden_of, zf1, up2_win)
        dz0 = run(add_round, g0, ds0)
        dza0 = gather_cols(dz0)
        gpre2_f0 = run(grad_pre_of, pre2_f0, gf0, down2_win)
        gpre2_f1 = run(grad_pre_of, pre2_f1, gf1, down2_win)
        acts2 = (za0, za1), (zf0, zf1)
        gpres2 = (win(after(gpre2_0, part1), 1), win(after(gpre2_1, part1), 1)), (gpre2_f0, gpre2_f1)
        sent = run(up_term, acts2, gpres2, 1 - row)
        got = swap(sent, "row")
        dz1 = run(add_round, g1, ds1)
        dza1 = gather_cols(dz1)
        up_b = run(up_term, acts2, gpres2, row, got)
        hids2 = (win(hid2_0, 1), win(hid2_1, 1)), (hid2_f0, hid2_f1)
        grads2 = (ga0, ga1), (gf0, gf1)
        sent = run(down_term, hids2, grads2, 1 - row)
        got = swap(sent, "row")
        dzf0 = swap(dza0, "dep")
        ys0 = scatter_cols(run(dot, hid2_0, down2))
        down_b = run(down_term, hids2, grads2, row, got)
        dzf1 = swap(after(dza1, down_b), "dep")
        down_b_moved = hop(after(down_b, dza1))
        ys1 = scatter_cols(run(dot, hid2_1, down2))

        gpre1_0 = run(grad_pre_of, pre1_0, dza0, down1)
        grad_up2 = join(after(up_b, gpre1_0), 1)
        xs0 = scatter_cols(run(dot_last, gpre1_0, up1))
        gpre1_1 = run(grad_pre_of, pre1_1, dza1, down1)
        grads1 = (dza0, dza1), (dzf0, dzf1)
        hids1 = (hid1_0, hid1_1), (hid1_f0[1], hid1_f1[1])
        sent = run(down_term, hids1, grads1, 1 - row)
        got = swap(sent, "row")
        xs1 = scatter_cols(run(dot_last, gpre1_1, up1))
        down_b = run(own_or, down_b, down_b_moved)
        grad_down2 = join(down_b, 0)
        down_a = run(down_term, hids1, grads1, row, got)
        half_a = hop(half_of(down_a, dep, 0))
        gpre1_f0 = run(grad_pre_of, hid1_f0[0], dzf0, down1)
        gpre1_f1 = run(grad_pre_of, hid1_f1[0], dzf1, down1)
        acts1 = (xa0, xa1), (xf0, xf1)
        gpres1 = (gpre1_0, gpre1_1), (gpre1_f0, gpre1_f1)
        sent = run(up_term, acts1, gpres1, 1 - row)
        got = swap(sent, "row")
        half_a_far = hop_far(after(half_a, sent))
        y0 = run(add_round, z0, ys0)
        y1 = run(add_round, z1, ys1)
        dx0 = run(add_round, dz0, xs0)
        grad_up1 = run(up_term, acts1, gpres1, row, got)
        dx1 = run(add_round, dz1, xs1)
        grad_down1 = own_or_halves(down_a, half_a, half_a_far)
        y_out = jnp.concatenate([y0, y1], axis=0)
        grad_x = jnp.concatenate([dx0, dx1], axis=0)
        return y_out, grad_x, grad_up1, grad_down1, grad_up2, grad_down2

    return jax.shard_map(local_step, mesh=mesh, in_specs=(act_spec, weight_spec, weight_spec, weight_spec, weight_spec, act_spec), out_specs=(act_spec, act_spec, weight_spec, weight_spec, weight_spec, weight_spec), check_vma=False)
```
